16 devices in a mesh: rep: 2 (over y, z), dp: 8 (over x, core).
Axes of the slice: x: 4, y: 2, z: 1, core: 2. Of those that a mesh axis runs over, the one named last changes fastest.
The devices are a block of a 4x4x8 slice.
Arguments:
- x: bfloat16 [16, 2048, 1024], P(('rep', 'dp')), parts along dimension 0
- dy: bfloat16 [16, 2048, 1024], P(('rep', 'dp')), parts along dimension 0
- w_gate: bfloat16 [2, 1024, 3200], P(None, 'dp')
- w_up: bfloat16 [2, 1024, 3200], P(None, 'dp')
- w_down: bfloat16 [2, 3200, 1024], P(None, 'dp')
Outputs:
- output 1: bfloat16 [16, 2048, 1024], P(('rep', 'dp')), parts along dimension 0
- output 2: bfloat16 [4, 1024, 3200], P('rep', 'dp'), parts along dimension 0
- output 3: bfloat16 [4, 1024, 3200], P('rep', 'dp'), parts along dimension 0
- output 4: bfloat16 [4, 3200, 1024], P('rep', 'dp'), parts along dimension 0
There are 2 independent parts. The reference program is written for one: setup_inputs(seed, part) draws one part's arguments, and reference() takes and returns one part's arrays. A program takes and returns all parts, laid end to end along the dimension named above; an argument that names none is the same for every part.
All inputs are finite; a program needn't handle non-finite values.
Results may differ from the reference program's by a relative error of at most 0.018.
Values are sent between devices in bfloat16 or wider.
A program may use at most 768 MiB of HBM per device.

```python
import jax
import jax.numpy as jnp
from jax import lax

SEQUENCES = 8
TOKENS = 2048
D = 1024
FF = 3200
LAYERS = 2
NAMES = ("w_gate", "w_up", "w_down")
SHAPES = {"w_gate": (LAYERS, D, FF), "w_up": (LAYERS, D, FF), "w_down": (LAYERS, FF, D)}


def bump(key, n, height):
    away = (jnp.arange(n, dtype=jnp.int32) - jax.random.randint(key, (), 0, n, jnp.int32)) % n
    return jnp.where(away < n // 8, height, 1.0)


def together(key, own, strength):
    shared = jax.random.normal(key, own.shape[1:], jnp.float32)
    return (own + strength * shared) * lax.rsqrt(1 + strength * strength)


def setup_inputs(seed: int = 0, part: int = 0) -> dict:
    kx, kdy, ka, kb, kz, kf, kh, kl, *kw = jax.random.split(jax.random.key(seed), 8 + len(NAMES))
    kx, kdy, ka, kb = (jax.random.fold_in(k, part) for k in (kx, kdy, ka, kb))
    shape = (SEQUENCES, TOKENS, D)
    much_x, much_dy = jax.random.uniform(kz, (2,), jnp.float32, 0.0, 1.0)
    layers = 2.0 ** jax.random.uniform(kl, (LAYERS, 1, 1), jnp.float32, -1.0, 1.0)
    x = together(ka, jax.random.normal(kx, shape, jnp.float32), much_x) * bump(kf, D, 4.0)
    dy = together(kb, jax.random.normal(kdy, shape, jnp.float32), much_dy)
    drawn = {"x": x.astype(jnp.bfloat16), "dy": (dy * (SEQUENCES * TOKENS) ** -0.5).astype(jnp.bfloat16)}
    for key, name in zip(kw, NAMES, strict=True):
        w = jax.random.normal(key, SHAPES[name], jnp.float32) * SHAPES[name][1] ** -0.5
        drawn[name] = (w * {"w_gate": 1.0, "w_up": bump(kh, FF, 4.0), "w_down": layers}[name]).astype(jnp.bfloat16)
    return drawn


def matmul(a, w):
    return jnp.dot(a, w, preferred_element_type=jnp.float32).astype(jnp.bfloat16)


def normed(h):
    wide = h.astype(jnp.float32)
    scale = lax.rsqrt(jnp.mean(wide**2, -1, keepdims=True) + 1e-6)
    return (wide * scale).astype(jnp.bfloat16)


def layer(h, w):
    a = normed(h)
    gate = jnp.dot(a, w["w_gate"], preferred_element_type=jnp.float32)
    up = jnp.dot(a, w["w_up"], preferred_element_type=jnp.float32)
    return h + matmul((jax.nn.silu(gate) * up).astype(jnp.bfloat16), w["w_down"])


def stack(weights, h):
    return lax.scan(lambda h, w: (layer(h, w), None), h, weights)[0]


def reference(x, dy, w_gate, w_up, w_down):
    weights = dict(zip(NAMES, (w_gate, w_up, w_down), strict=True))

    def take(so_far, sequence):
        h, by_y = sequence
        _, back = jax.vjp(stack, weights, h)
        by_weights, by_h = back(by_y)
        return jax.tree.map(lambda total, term: total + term.astype(jnp.float32), so_far, by_weights), by_h

    none_yet = {name: jnp.zeros(w.shape, jnp.float32) for name, w in weights.items()}
    by_weights, by_x = lax.scan(take, none_yet, (x, dy))
    return (by_x, *(by_weights[name].astype(jnp.bfloat16) for name in NAMES))
```

```python
import functools

import jax
import jax.numpy as jnp
from jax import lax
from jax.experimental import pallas as pl
from jax.experimental.pallas import tpu as pltpu
from jax.sharding import PartitionSpec as P

F32 = jnp.float32
BF = jnp.bfloat16
VMEM_LIMIT = 60 * 1024 * 1024
ANY = pl.BlockSpec(memory_space=pl.ANY)
EPS = 1e-6


def dot(a, b, ca=1, cb=0):
    return lax.dot_general(a, b, (((ca,), (cb,)), ((), ())), preferred_element_type=F32)


def rounded(v):
    return v.astype(BF).astype(F32)


def whole(shape):
    return pl.BlockSpec(shape, lambda *_: (0,) * len(shape), pipeline_mode=pl.Buffered(1))


def params(dims):
    return pltpu.CompilerParams(dimension_semantics=("arbitrary",) * dims, vmem_limit_bytes=VMEM_LIMIT)


def cost(flops, nbytes):
    return pl.CostEstimate(flops=int(flops), bytes_accessed=int(nbytes), transcendentals=0)


def normed(h):
    wide = h.astype(F32)
    return (wide * lax.rsqrt(jnp.mean(wide * wide, -1, keepdims=True) + EPS)).astype(BF)


KINDS = 11


def forward_kernel(n, *refs):
    x_ref, *stacked = refs[:4]
    shards = [w.at[number] for number in range(2) for w in stacked]
    gathered = refs[4:10]
    a0_ref, act_ref, h1_ref, a1_ref = refs[10:14]
    own = refs[14:20]
    x_v, a_v, act_v, wd_v, w_buf, send, recv, load, store, w_sem, act_sem, row_sem = refs[20:]
    T, D = x_ref.shape
    FF = shards[0].shape[1]
    r, i = lax.axis_index("rep"), lax.axis_index("dp")
    nx = n // 2
    x, c = lax.div(i, 2), lax.rem(i, 2)
    q = lax.rem(r, 2)
    s = 1 - 2 * q
    h = 1 - q
    xa = lax.rem(x + s + nx, nx)
    xb = lax.rem(x - s + nx, nx)
    x2 = lax.rem(x + 2, nx)
    to_a, to_b, to_pair, to_core = (r, 2 * xa + c), (r, 2 * xb + c), (r + s, i), (r, 2 * x + 1 - c)

    barrier = pltpu.get_barrier_semaphore()
    for who in (to_a, to_b, to_pair, to_core):
        pl.semaphore_signal(barrier, inc=1, device_id=who, device_id_type=pl.DeviceIdType.MESH)

    def part(ref, base, half):
        rows = shards[0].shape[0] if ref.shape[1] == FF else shards[2].shape[0]
        if ref.shape[1] == FF:
            if half is None:
                return ref.at[pl.ds(pl.multiple_of(base * rows, rows), rows), :]
            return ref.at[pl.ds(pl.multiple_of(base * rows + half * (rows // 2), rows // 2), rows // 2), :]
        at = pl.ds(pl.multiple_of(base * rows, 16), rows)
        if half is None:
            return ref.at[at, :]
        return ref.at[at, pl.ds(pl.multiple_of(half * (D // 2), D // 2), D // 2)]

    def copy(p, kind, arriving=False):
        w = gathered[p]
        src = None
        if kind == 0:
            where, half, there, lands, lhalf, lcore = x, None, to_a, xb, None, c
        elif kind == 1:
            where, half, there, lands, lhalf, lcore = x, h, to_b, xa, h, c
        elif kind == 2:
            where, half, there, lands, lhalf, lcore = xa, h, to_b, x2, h, c
        elif kind == 3:
            where, half, there, lands, lhalf, lcore = xb, h, to_pair, xa, 1 - h, c
        elif kind == 4:
            where, half, there, lands, lhalf, lcore = x2, h, to_pair, x2, 1 - h, c
        else:
            where, half = ((x, None), (xb, None), (xa, h), (x2, h), (xa, 1 - h), (x2, 1 - h))[kind - 5]
            there, lands, lhalf, lcore = to_core, where, half, 1 - c
        dst = part(w, 2 * where + c, half)
        if kind in (0, 1, 5):
            src = part(own[p], 0, half)
        else:
            src = dst
        if arriving:
            src = dst = part(w, 2 * lands + lcore, lhalf)
        return pltpu.make_async_remote_copy(src_ref=src, dst_ref=dst, send_sem=send.at[p, kind], recv_sem=recv.at[p, kind],
                                            device_id=there, device_id_type=pl.DeviceIdType.MESH)

    def go(p, *kinds):
        for k in kinds:
            copy(p, k).start()

    def got(p, *kinds):
        for k in kinds:
            copy(p, k, True).wait_recv()

    def loads(p):
        return pltpu.make_async_copy(shards[p], own[p], load.at[p])

    def stores(p):
        return pltpu.make_async_copy(own[p], part(gathered[p], i, None), store.at[p])

    for p in range(6):
        loads(p).start()

    def start(p):
        loads(p).wait()
        go(p, 1, 0, 5)
        stores(p).start()

    def mid(p):
        got(p, 1)
        go(p, 2)
        got(p, 0)
        go(p, 3, 6, 7)

    def late(p):
        got(p, 2)
        go(p, 4, 8)
        got(p, 3)
        go(p, 9)

    def last(p):
        got(p, 4)
        go(p, 10)

    def done(p):
        got(p, 5, 6, 7, 8, 9, 10)
        stores(p).wait()

    x_load = pltpu.make_async_copy(x_ref, x_v, row_sem.at[0])
    x_load.start()
    pl.semaphore_wait(barrier, 4)
    start(0)
    start(1)

    mt, ft = 256, 256
    full = FF // ft
    rest = FF - full * ft
    x_load.wait()

    def rows_at(m):
        return pl.ds(pl.multiple_of(m * mt, mt), mt)

    @pl.loop(0, T // mt)
    def _(m):
        a_v[rows_at(m), :] = normed(x_v[rows_at(m), :])

    a_out = pltpu.make_async_copy(a_v, a0_ref, row_sem.at[0])
    a_out.start()

    def columns(t, width):
        return pl.ds(pl.multiple_of(t * ft, ft), width)

    def w_copies(t, slot, width):
        return [pltpu.make_async_copy(gathered[k].at[:, columns(t, width)], w_buf.at[k, slot, :, pl.ds(0, width)], w_sem.at[k, slot])
                for k in range(2)]

    def act_out(t, width):
        return pltpu.make_async_copy(act_v.at[:, columns(t, width)], act_ref.at[:, columns(t, width)], act_sem.at[t])

    def act_tile(t, slot, width):
        for cp in w_copies(t, slot, width):
            cp.wait()

        @pl.when(t + 1 < full)
        def _():
            for cp in w_copies(t + 1, 1 - slot, ft):
                cp.start()

        if rest and width == ft:
            @pl.when(t + 1 == full)
            def _():
                for cp in w_copies(t + 1, 1 - slot, rest):
                    cp.start()

        wg_t, wu_t = w_buf[0, slot, :, :width], w_buf[1, slot, :, :width]
        for m in range(T // mt):
            rows = pl.ds(m * mt, mt)
            a = a_v[rows, :]
            g, u = dot(a, wg_t), dot(a, wu_t)
            act_v[rows, columns(t, width)] = (g * jax.nn.sigmoid(g) * u).astype(BF)
        act_out(t, width).start()

    def gate_up(first, last):
        @pl.loop(first, last)
        def _(t):
            act_tile(t, lax.rem(t, 2), ft)

    def down(first, last):
        @pl.loop(first, last)
        def _(m):
            y = dot(act_v[rows_at(m), :], wd_v[...])
            hh = (x_v[rows_at(m), :].astype(F32) + rounded(y)).astype(BF)
            x_v[rows_at(m), :] = hh
            a_v[rows_at(m), :] = normed(hh)

    mid(0)
    start(2)
    late(0)
    mid(1)
    start(3)
    last(0)
    late(1)
    mid(2)
    start(4)
    last(1)
    done(0)
    done(1)
    for cp in w_copies(0, 0, ft):
        cp.start()
    gate_up(0, 3)
    late(2)
    gate_up(3, 7)
    last(2)
    gate_up(7, 9)
    mid(3)
    start(5)
    gate_up(9, full)
    done(2)
    wd_load = pltpu.make_async_copy(gathered[2], wd_v, row_sem.at[1])
    wd_load.start()
    if rest:
        act_tile(full, full % 2, rest)
    late(3)
    a_out.wait()
    wd_load.wait()
    down(0, 2)
    last(3)
    down(2, 4)
    mid(4)
    down(4, T // mt)
    h_out = pltpu.make_async_copy(x_v, h1_ref, row_sem.at[0])
    h_out.start()
    a1_out = pltpu.make_async_copy(a_v, a1_ref, row_sem.at[1])
    a1_out.start()
    late(4)
    mid(5)
    last(4)
    late(5)
    last(5)
    done(3)
    done(4)
    done(5)
    for t in range(full + (rest > 0)):
        act_out(t, ft if t < full else rest).wait()
    h_out.wait()
    a1_out.wait()
    for p in range(6):
        for k in range(KINDS):
            copy(p, k).wait_send()


def forward(n, x, stacked):
    T, D = x.shape
    shards = [jax.ShapeDtypeStruct(w.shape[1:], BF) for _ in range(2) for w in stacked]
    FF = shards[0].shape[1]
    fulls = [jax.ShapeDtypeStruct((w.shape[0] * n, w.shape[1]), BF) for w in shards]
    wide = jax.ShapeDtypeStruct((T, D), BF)
    return pl.pallas_call(
        functools.partial(forward_kernel, n),
        name="gather_forward",
        out_shape=[*fulls, wide, jax.ShapeDtypeStruct((T, FF), BF), wide, wide],
        in_specs=[ANY] * 4,
        out_specs=[ANY] * 10,
        scratch_shapes=[
            *[pltpu.VMEM(w.shape, BF) for w in shards],
            pltpu.VMEM((T, D), BF),
            pltpu.VMEM((T, D), BF),
            pltpu.VMEM((T, FF), BF),
            pltpu.VMEM((FF, D), BF),
            pltpu.VMEM((2, 2, D, 256), BF),
            pltpu.SemaphoreType.DMA((6, KINDS)),
            pltpu.SemaphoreType.DMA((6, KINDS)),
            pltpu.SemaphoreType.DMA((6,)),
            pltpu.SemaphoreType.DMA((6,)),
            pltpu.SemaphoreType.DMA((2, 2)),
            pltpu.SemaphoreType.DMA((pl.cdiv(FF, 256),)),
            pltpu.SemaphoreType.DMA((2,)),
        ],
        compiler_params=pltpu.CompilerParams(collective_id=0, has_side_effects=True, vmem_limit_bytes=VMEM_LIMIT),
        cost_estimate=cost(6 * T * D * FF, 2e8),
    )(x, *stacked)


def inner_backward(a, dy, wg, wu, wd, keep_act):
    T, D = a.shape
    FF = wg.shape[1]
    ft, sub = 256, 256

    def body(a_ref, dy_ref, wg_ref, wu_ref, wd_ref, *outs):
        dg_ref, du_ref = outs[-2:]
        for m in range(T // sub):
            rows = pl.ds(m * sub, sub)
            av = a_ref[rows, :]
            g, u = dot(av, wg_ref[...]), dot(av, wu_ref[...])
            d = rounded(dot(dy_ref[rows, :], wd_ref[...], 1, 1))
            sg = jax.nn.sigmoid(g)
            sl = g * sg
            if keep_act:
                outs[0][rows, :] = (sl * u).astype(BF)
            du_ref[rows, :] = (d * sl).astype(BF)
            dg_ref[rows, :] = (d * u * (sg + sl * (1.0 - sg))).astype(BF)

    col = pl.BlockSpec((D, ft), lambda j: (0, j))
    out = pl.BlockSpec((T, ft), lambda j: (0, j))
    count = 3 if keep_act else 2
    return pl.pallas_call(
        body, name="inner_backward", grid=(pl.cdiv(FF, ft),),
        in_specs=[whole((T, D)), whole((T, D)), col, col, pl.BlockSpec((ft, D), lambda j: (j, 0))],
        out_specs=[out] * count, out_shape=[jax.ShapeDtypeStruct((T, FF), BF)] * count,
        compiler_params=params(1), cost_estimate=cost(6 * T * D * FF, 6e7),
    )(a, dy, wg, wu, wd)


def down_grad(act, dy):
    T, FF = act.shape
    D = dy.shape[1]
    ft = 640

    def body(a_ref, b_ref, o_ref):
        o_ref[...] = dot(a_ref[...], b_ref[...], 0, 0).astype(BF)

    return pl.pallas_call(
        body, name="down_grad", grid=(FF // ft,),
        in_specs=[pl.BlockSpec((T, ft), lambda j: (0, j)), whole((T, D))],
        out_specs=pl.BlockSpec((ft, D), lambda j: (j, 0)), out_shape=jax.ShapeDtypeStruct((FF, D), BF),
        compiler_params=params(1), cost_estimate=cost(2 * T * D * FF, 3e7),
    )(act, dy)


def up_grad(a, dup):
    T, D = a.shape
    FF = dup.shape[1]
    ft = 512

    def body(a_ref, b_ref, o_ref):
        o_ref[...] = dot(a_ref[...], b_ref[...], 0, 0).astype(BF)

    return pl.pallas_call(
        body, name="up_grad", grid=(pl.cdiv(FF, ft),),
        in_specs=[whole((T, D)), pl.BlockSpec((T, ft), lambda j: (0, j))],
        out_specs=pl.BlockSpec((D, ft), lambda j: (0, j)), out_shape=jax.ShapeDtypeStruct((D, FF), BF),
        compiler_params=params(1), cost_estimate=cost(2 * T * D * FF, 3e7),
    )(a, dup)


def input_grad(dgate, dup, wg, wu, h, dh):
    T, FF = dgate.shape
    D = wg.shape[0]
    mt = 256

    def body(g_ref, u_ref, wg_ref, wu_ref, h_ref, dh_ref, o_ref):
        p = rounded(dot(g_ref[...], wg_ref[...], 1, 1))
        q = rounded(dot(u_ref[...], wu_ref[...], 1, 1))
        d = rounded(p + q)
        w = h_ref[...].astype(F32)
        sc = lax.rsqrt(jnp.mean(w * w, -1, keepdims=True) + EPS)
        ds = jnp.sum(d * w, -1, keepdims=True)
        dw = d * sc - w * (ds * sc * sc * sc * (1.0 / D))
        o_ref[...] = (dh_ref[...].astype(F32) + rounded(dw)).astype(BF)

    tf, td = pl.BlockSpec((mt, FF), lambda m: (m, 0)), pl.BlockSpec((mt, D), lambda m: (m, 0))
    return pl.pallas_call(
        body, name="input_grad", grid=(T // mt,), in_specs=[tf, tf, whole((D, FF)), whole((D, FF)), td, td], out_specs=td,
        out_shape=jax.ShapeDtypeStruct((T, D), BF), compiler_params=params(1), cost_estimate=cost(4 * T * D * FF, 5e7),
    )(dgate, dup, wg, wu, h, dh)


def after(value, *others):
    return lax.optimization_barrier((value, *others))[0]


def solution(mesh):
    n = mesh.shape["dp"]

    def step(x, dy, wg, wu, wd):
        x, dy = x[0], dy[0]
        *full, a0, act0, h1, a1 = forward(n, x, (wg, wu, wd))

        def scattered(t):
            return lax.psum_scatter(t, "dp", scatter_dimension=0, tiled=True)

        act1, dg1, du1 = inner_backward(a1, dy, *full[3:], True)
        dwd1 = down_grad(act1, dy)
        sd1 = scattered(dwd1)
        dwg1 = up_grad(a1, after(dg1, dwd1))
        sg1 = scattered(dwg1)
        dwu1 = up_grad(a1, after(du1, dwg1))
        su1 = scattered(dwu1)
        dh1 = input_grad(after(dg1, dwu1, sd1), du1, full[3], full[4], h1, dy)
        dwd0 = down_grad(act0, after(dh1, sg1))
        sd0 = scattered(dwd0)
        dg0, du0 = inner_backward(a0, after(dh1, dwd0), *full[:3], False)
        dwg0 = up_grad(a0, after(dg0, su1))
        sg0 = scattered(dwg0)
        dwu0 = up_grad(a0, after(du0, dwg0))
        su0 = scattered(dwu0)
        dx = input_grad(after(dg0, dwu0), du0, full[0], full[1], x, dh1)
        return dx[None], jnp.stack([sg0, sg1]), jnp.stack([su0, su1]), jnp.stack([sd0, sd1])

    w = P(None, "dp", None)
    return jax.shard_map(
        step, mesh=mesh,
        in_specs=(P(("rep", "dp")), P(("rep", "dp")), w, w, w),
        out_specs=(P(("rep", "dp")), P("rep", "dp"), P("rep", "dp"), P("rep", "dp")),
        check_vma=False,
    )
```

```python
import functools

import jax
import jax.numpy as jnp
from jax import lax
from jax.experimental import pallas as pl
from jax.experimental.pallas import tpu as pltpu
from jax.sharding import PartitionSpec as P

F32 = jnp.float32
BF = jnp.bfloat16
VMEM_LIMIT = 60 * 1024 * 1024
ANY = pl.BlockSpec(memory_space=pl.ANY)
EPS = 1e-6


def dot(a, b, ca=1, cb=0):
    return lax.dot_general(a, b, (((ca,), (cb,)), ((), ())), preferred_element_type=F32)


def rounded(v):
    return v.astype(BF).astype(F32)


def whole(shape):
    return pl.BlockSpec(shape, lambda *_: (0,) * len(shape), pipeline_mode=pl.Buffered(1))


def params(dims):
    return pltpu.CompilerParams(dimension_semantics=("arbitrary",) * dims, vmem_limit_bytes=VMEM_LIMIT)


def cost(flops, nbytes):
    return pl.CostEstimate(flops=int(flops), bytes_accessed=int(nbytes), transcendentals=0)


def normed(h):
    wide = h.astype(F32)
    return (wide * lax.rsqrt(jnp.mean(wide * wide, -1, keepdims=True) + EPS)).astype(BF)


KINDS = 11


def forward_kernel(n, *refs):
    x_ref, *stacked = refs[:4]
    shards = [w.at[number] for number in range(2) for w in stacked]
    gathered = refs[4:10]
    a0_ref, act_ref, h1_ref, a1_ref = refs[10:14]
    own = refs[14:20]
    x_v, a_v, act_v, wd_v, w_buf, send, recv, load, store, w_sem, act_sem, row_sem = refs[20:]
    T, D = x_ref.shape
    FF = shards[0].shape[1]
    r, i = lax.axis_index("rep"), lax.axis_index("dp")
    nx = n // 2
    x, c = lax.div(i, 2), lax.rem(i, 2)
    q = lax.rem(r, 2)
    s = 1 - 2 * q
    h = 1 - q
    xa = lax.rem(x + s + nx, nx)
    xb = lax.rem(x - s + nx, nx)
    x2 = lax.rem(x + 2, nx)
    to_a, to_b, to_pair, to_core = (r, 2 * xa + c), (r, 2 * xb + c), (r + s, i), (r, 2 * x + 1 - c)

    barrier = pltpu.get_barrier_semaphore()
    for who in (to_a, to_b, to_pair, to_core):
        pl.semaphore_signal(barrier, inc=1, device_id=who, device_id_type=pl.DeviceIdType.MESH)

    def part(ref, base, half):
        rows = shards[0].shape[0] if ref.shape[1] == FF else shards[2].shape[0]
        if ref.shape[1] == FF:
            if half is None:
                return ref.at[pl.ds(pl.multiple_of(base * rows, rows), rows), :]
            return ref.at[pl.ds(pl.multiple_of(base * rows + half * (rows // 2), rows // 2), rows // 2), :]
        at = pl.ds(pl.multiple_of(base * rows, 16), rows)
        if half is None:
            return ref.at[at, :]
        return ref.at[at, pl.ds(pl.multiple_of(half * (D // 2), D // 2), D // 2)]

    def copy(p, kind, arriving=False):
        w = gathered[p]
        src = None
        if kind == 0:
            where, half, there, lands, lhalf, lcore = x, None, to_a, xb, None, c
        elif kind == 1:
            where, half, there, lands, lhalf, lcore = x, h, to_b, xa, h, c
        elif kind == 2:
            where, half, there, lands, lhalf, lcore = xa, h, to_b, x2, h, c
        elif kind == 3:
            where, half, there, lands, lhalf, lcore = xb, h, to_pair, xa, 1 - h, c
        elif kind == 4:
            where, half, there, lands, lhalf, lcore = x2, h, to_pair, x2, 1 - h, c
        else:
            where, half = ((x, None), (xb, None), (xa, h), (x2, h), (xa, 1 - h), (x2, 1 - h))[kind - 5]
            there, lands, lhalf, lcore = to_core, where, half, 1 - c
        dst = part(w, 2 * where + c, half)
        if kind in (0, 1, 5):
            src = part(own[p], 0, half)
        else:
            src = dst
        if arriving:
            src = dst = part(w, 2 * lands + lcore, lhalf)
        return pltpu.make_async_remote_copy(src_ref=src, dst_ref=dst, send_sem=send.at[p, kind], recv_sem=recv.at[p, kind],
                                            device_id=there, device_id_type=pl.DeviceIdType.MESH)

    def go(p, *kinds):
        for k in kinds:
            copy(p, k).start()

    def got(p, *kinds):
        for k in kinds:
            copy(p, k, True).wait_recv()

    def loads(p):
        return pltpu.make_async_copy(shards[p], own[p], load.at[p])

    def stores(p):
        return pltpu.make_async_copy(own[p], part(gathered[p], i, None), store.at[p])

    for p in range(6):
        loads(p).start()

    def start(p):
        loads(p).wait()
        go(p, 1, 0, 5)
        stores(p).start()

    def mid(p):
        got(p, 1)
        go(p, 2)
        got(p, 0)
        go(p, 3, 6, 7)

    def late(p):
        got(p, 2)
        go(p, 4, 8)
        got(p, 3)
        go(p, 9)

    def last(p):
        got(p, 4)
        go(p, 10)

    def done(p):
        got(p, 5, 6, 7, 8, 9, 10)
        stores(p).wait()

    x_load = pltpu.make_async_copy(x_ref, x_v, row_sem.at[0])
    x_load.start()
    pl.semaphore_wait(barrier, 4)
    start(0)
    start(1)

    mt, ft = 256, 256
    full = FF // ft
    rest = FF - full * ft
    x_load.wait()

    def rows_at(m):
        return pl.ds(pl.multiple_of(m * mt, mt), mt)

    @pl.loop(0, T // mt)
    def _(m):
        a_v[rows_at(m), :] = normed(x_v[rows_at(m), :])

    a_out = pltpu.make_async_copy(a_v, a0_ref, row_sem.at[0])
    a_out.start()

    def columns(t, width):
        return pl.ds(pl.multiple_of(t * ft, ft), width)

    def w_copies(t, slot, width):
        return [pltpu.make_async_copy(gathered[k].at[:, columns(t, width)], w_buf.at[k, slot, :, pl.ds(0, width)], w_sem.at[k, slot])
                for k in range(2)]

    def act_out(t, width):
        return pltpu.make_async_copy(act_v.at[:, columns(t, width)], act_ref.at[:, columns(t, width)], act_sem.at[t])

    def act_tile(t, slot, width):
        for cp in w_copies(t, slot, width):
            cp.wait()

        @pl.when(t + 1 < full)
        def _():
            for cp in w_copies(t + 1, 1 - slot, ft):
                cp.start()

        if rest and width == ft:
            @pl.when(t + 1 == full)
            def _():
                for cp in w_copies(t + 1, 1 - slot, rest):
                    cp.start()

        wg_t, wu_t = w_buf[0, slot, :, :width], w_buf[1, slot, :, :width]
        for m in range(T // mt):
            rows = pl.ds(m * mt, mt)
            a = a_v[rows, :]
            g, u = dot(a, wg_t), dot(a, wu_t)
            act_v[rows, columns(t, width)] = (g * jax.nn.sigmoid(g) * u).astype(BF)
        act_out(t, width).start()

    def gate_up(first, last):
        @pl.loop(first, last)
        def _(t):
            act_tile(t, lax.rem(t, 2), ft)

    def down(first, last):
        @pl.loop(first, last)
        def _(m):
            y = dot(act_v[rows_at(m), :], wd_v[...])
            hh = (x_v[rows_at(m), :].astype(F32) + rounded(y)).astype(BF)
            x_v[rows_at(m), :] = hh
            a_v[rows_at(m), :] = normed(hh)

    mid(0)
    start(2)
    late(0)
    mid(1)
    start(3)
    last(0)
    late(1)
    mid(2)
    start(4)
    last(1)
    done(0)
    done(1)
    for cp in w_copies(0, 0, ft):
        cp.start()
    gate_up(0, 3)
    late(2)
    gate_up(3, 7)
    last(2)
    gate_up(7, 8)
    mid(3)
    start(5)
    gate_up(8, 11)
    late(3)
    gate_up(11, full)
    done(2)
    wd_load = pltpu.make_async_copy(gathered[2], wd_v, row_sem.at[1])
    wd_load.start()
    if rest:
        act_tile(full, full % 2, rest)
    last(3)
    mid(4)
    a_out.wait()
    wd_load.wait()
    down(0, 5)
    late(4)
    down(5, T // mt)
    h_out = pltpu.make_async_copy(x_v, h1_ref, row_sem.at[0])
    h_out.start()
    a1_out = pltpu.make_async_copy(a_v, a1_ref, row_sem.at[1])
    a1_out.start()
    mid(5)
    last(4)
    late(5)
    last(5)
    done(3)
    done(4)
    done(5)
    for t in range(full + (rest > 0)):
        act_out(t, ft if t < full else rest).wait()
    h_out.wait()
    a1_out.wait()
    for p in range(6):
        for k in range(KINDS):
            copy(p, k).wait_send()


def forward(n, x, stacked):
    T, D = x.shape
    shards = [jax.ShapeDtypeStruct(w.shape[1:], BF) for _ in range(2) for w in stacked]
    FF = shards[0].shape[1]
    fulls = [jax.ShapeDtypeStruct((w.shape[0] * n, w.shape[1]), BF) for w in shards]
    wide = jax.ShapeDtypeStruct((T, D), BF)
    return pl.pallas_call(
        functools.partial(forward_kernel, n),
        name="gather_forward",
        out_shape=[*fulls, wide, jax.ShapeDtypeStruct((T, FF), BF), wide, wide],
        in_specs=[ANY] * 4,
        out_specs=[ANY] * 10,
        scratch_shapes=[
            *[pltpu.VMEM(w.shape, BF) for w in shards],
            pltpu.VMEM((T, D), BF),
            pltpu.VMEM((T, D), BF),
            pltpu.VMEM((T, FF), BF),
            pltpu.VMEM((FF, D), BF),
            pltpu.VMEM((2, 2, D, 256), BF),
            pltpu.SemaphoreType.DMA((6, KINDS)),
            pltpu.SemaphoreType.DMA((6, KINDS)),
            pltpu.SemaphoreType.DMA((6,)),
            pltpu.SemaphoreType.DMA((6,)),
            pltpu.SemaphoreType.DMA((2, 2)),
            pltpu.SemaphoreType.DMA((pl.cdiv(FF, 256),)),
            pltpu.SemaphoreType.DMA((2,)),
        ],
        compiler_params=pltpu.CompilerParams(collective_id=0, has_side_effects=True, vmem_limit_bytes=VMEM_LIMIT),
        cost_estimate=cost(6 * T * D * FF, 2e8),
    )(x, *stacked)


def inner_backward(a, dy, wg, wu, wd, keep_act):
    T, D = a.shape
    FF = wg.shape[1]
    ft, sub = 256, 256

    def body(a_ref, dy_ref, wg_ref, wu_ref, wd_ref, *outs):
        dg_ref, du_ref = outs[-2:]
        for m in range(T // sub):
            rows = pl.ds(m * sub, sub)
            av = a_ref[rows, :]
            g, u = dot(av, wg_ref[...]), dot(av, wu_ref[...])
            d = rounded(dot(dy_ref[rows, :], wd_ref[...], 1, 1))
            sg = jax.nn.sigmoid(g)
            sl = g * sg
            if keep_act:
                outs[0][rows, :] = (sl * u).astype(BF)
            du_ref[rows, :] = (d * sl).astype(BF)
            dg_ref[rows, :] = (d * u * (sg + sl * (1.0 - sg))).astype(BF)

    col = pl.BlockSpec((D, ft), lambda j: (0, j))
    out = pl.BlockSpec((T, ft), lambda j: (0, j))
    count = 3 if keep_act else 2
    return pl.pallas_call(
        body, name="inner_backward", grid=(pl.cdiv(FF, ft),),
        in_specs=[whole((T, D)), whole((T, D)), col, col, pl.BlockSpec((ft, D), lambda j: (j, 0))],
        out_specs=[out] * count, out_shape=[jax.ShapeDtypeStruct((T, FF), BF)] * count,
        compiler_params=params(1), cost_estimate=cost(6 * T * D * FF, 6e7),
    )(a, dy, wg, wu, wd)


def down_grad(act, dy):
    T, FF = act.shape
    D = dy.shape[1]
    ft = 640

    def body(a_ref, b_ref, o_ref):
        o_ref[...] = dot(a_ref[...], b_ref[...], 0, 0).astype(BF)

    return pl.pallas_call(
        body, name="down_grad", grid=(FF // ft,),
        in_specs=[pl.BlockSpec((T, ft), lambda j: (0, j)), whole((T, D))],
        out_specs=pl.BlockSpec((ft, D), lambda j: (j, 0)), out_shape=jax.ShapeDtypeStruct((FF, D), BF),
        compiler_params=params(1), cost_estimate=cost(2 * T * D * FF, 3e7),
    )(act, dy)


def up_grad(a, dup):
    T, D = a.shape
    FF = dup.shape[1]
    ft = 512

    def body(a_ref, b_ref, o_ref):
        o_ref[...] = dot(a_ref[...], b_ref[...], 0, 0).astype(BF)

    return pl.pallas_call(
        body, name="up_grad", grid=(pl.cdiv(FF, ft),),
        in_specs=[whole((T, D)), pl.BlockSpec((T, ft), lambda j: (0, j))],
        out_specs=pl.BlockSpec((D, ft), lambda j: (0, j)), out_shape=jax.ShapeDtypeStruct((D, FF), BF),
        compiler_params=params(1), cost_estimate=cost(2 * T * D * FF, 3e7),
    )(a, dup)


def input_grad(dgate, dup, wg, wu, h, dh):
    T, FF = dgate.shape
    D = wg.shape[0]
    mt = 256

    def body(g_ref, u_ref, wg_ref, wu_ref, h_ref, dh_ref, o_ref, wg_v, wu_v, sem):
        loads = [pltpu.make_async_copy(wg_ref, wg_v, sem.at[0]), pltpu.make_async_copy(wu_ref, wu_v, sem.at[1])]
        first = pl.program_id(0) == 0

        @pl.when(first)
        def _():
            loads[0].start()
            loads[1].start()
            loads[0].wait()

        p = rounded(dot(g_ref[...], wg_v[...], 1, 1))

        @pl.when(first)
        def _():
            loads[1].wait()

        q = rounded(dot(u_ref[...], wu_v[...], 1, 1))
        d = rounded(p + q)
        w = h_ref[...].astype(F32)
        sc = lax.rsqrt(jnp.mean(w * w, -1, keepdims=True) + EPS)
        ds = jnp.sum(d * w, -1, keepdims=True)
        dw = d * sc - w * (ds * sc * sc * sc * (1.0 / D))
        o_ref[...] = (dh_ref[...].astype(F32) + rounded(dw)).astype(BF)

    tf, td = pl.BlockSpec((mt, FF), lambda m: (m, 0)), pl.BlockSpec((mt, D), lambda m: (m, 0))
    return pl.pallas_call(
        body, name="input_grad", grid=(T // mt,), in_specs=[tf, tf, ANY, ANY, td, td], out_specs=td,
        scratch_shapes=[pltpu.VMEM((D, FF), BF), pltpu.VMEM((D, FF), BF), pltpu.SemaphoreType.DMA((2,))],
        out_shape=jax.ShapeDtypeStruct((T, D), BF), compiler_params=params(1), cost_estimate=cost(4 * T * D * FF, 5e7),
    )(dgate, dup, wg, wu, h, dh)


def after(value, *others):
    return lax.optimization_barrier((value, *others))[0]


def solution(mesh):
    n = mesh.shape["dp"]

    def step(x, dy, wg, wu, wd):
        x, dy = x[0], dy[0]
        *full, a0, act0, h1, a1 = forward(n, x, (wg, wu, wd))

        def scattered(t):
            return lax.psum_scatter(t, "dp", scatter_dimension=0, tiled=True)

        act1, dg1, du1 = inner_backward(a1, dy, *full[3:], True)
        dwd1 = down_grad(act1, dy)
        sd1 = scattered(dwd1)
        dwg1 = up_grad(a1, after(dg1, dwd1))
        sg1 = scattered(dwg1)
        dwu1 = up_grad(a1, after(du1, dwg1))
        su1 = scattered(dwu1)
        dh1 = input_grad(after(dg1, dwu1, sd1), du1, full[3], full[4], h1, dy)
        dwd0 = down_grad(act0, after(dh1, sg1))
        sd0 = scattered(dwd0)
        dg0, du0 = inner_backward(a0, after(dh1, dwd0), *full[:3], False)
        dwg0 = up_grad(a0, after(dg0, su1))
        sg0 = scattered(dwg0)
        dwu0 = up_grad(a0, after(du0, dwg0))
        su0 = scattered(dwu0)
        dx = input_grad(after(dg0, dwu0), du0, full[0], full[1], x, dh1)
        return dx[None], jnp.stack([sg0, sg1]), jnp.stack([su0, su1]), jnp.stack([sd0, sd1])

    w = P(None, "dp", None)
    return jax.shard_map(
        step, mesh=mesh,
        in_specs=(P(("rep", "dp")), P(("rep", "dp")), w, w, w),
        out_specs=(P(("rep", "dp")), P("rep", "dp"), P("rep", "dp"), P("rep", "dp")),
        check_vma=False,
    )
```
